16 devices in a mesh: dp: 2 (over z), tp: 8 (over y, x, core).
Axes of the slice: x: 2, y: 2, z: 2, core: 2. Of those that a mesh axis runs over, the one named last changes fastest.
Arguments:
- hidden_in: bfloat16 [2048, 4096], P(('dp', 'tp')), parts along dimension 0
- k_cache: bfloat16 [2048, 512, 256], P(('dp', 'tp')), parts along dimension 0
- v_cache: bfloat16 [2048, 512, 256], P(('dp', 'tp')), parts along dimension 0
- cache_len: int32 [2048], P(('dp', 'tp')), parts along dimension 0
- norm_attn: bfloat16 [4096], replicated
- norm_mlp: bfloat16 [4096], replicated
- w_q: bfloat16 [4096, 4096], replicated
- w_k: bfloat16 [4096, 256], replicated
- w_v: bfloat16 [4096, 256], replicated
- w_o: bfloat16 [4096, 4096], replicated
- w_gate: bfloat16 [4096, 16384], P(None, 'tp')
- w_up: bfloat16 [4096, 16384], P(None, 'tp')
- w_down: bfloat16 [16384, 4096], P('tp')
Outputs:
- output 1: bfloat16 [2048, 4096], P(('dp', 'tp')), parts along dimension 0
- output 2: bfloat16 [2048, 256], P(('dp', 'tp')), parts along dimension 0
- output 3: bfloat16 [2048, 256], P(('dp', 'tp')), parts along dimension 0
There are 2 independent parts. The reference program is written for one: setup_inputs(seed, part) draws one part's arguments, and reference() takes and returns one part's arrays. A program takes and returns all parts, laid end to end along the dimension named above; an argument that names none is the same for every part.
All inputs are finite; a program needn't handle non-finite values.
Results may differ from the reference program's by a relative error of at most 0.0059934.
Values are sent between devices in bfloat16 or wider.
A program may use at most 1 GiB of HBM per device.

```python
import jax
import jax.numpy as jnp
from jax import lax

D_MODEL = 4096
NUM_HEADS = 16
HEAD_DIM = 256
FF_DIM = 16384
BATCH_ROWS = 1024
CACHE_SIZE = 512


def scaled_normal(key_w, shape_w, fan_in):
    return (jax.random.normal(key_w, shape_w, jnp.float32) * fan_in ** -0.5).astype(jnp.bfloat16)


def setup_inputs(seed: int = 0, part: int = 0) -> dict:
    base_key = jax.random.key(seed)
    shared_keys = jax.random.split(base_key, 9)
    own_keys = jax.random.split(jax.random.fold_in(base_key, part), 5)
    q_width = NUM_HEADS * HEAD_DIM
    hidden_in = jax.random.normal(own_keys[0], (BATCH_ROWS, D_MODEL), jnp.float32)
    k_cache = 2.0 * jax.random.normal(own_keys[1], (BATCH_ROWS, CACHE_SIZE, HEAD_DIM), jnp.float32)
    v_mean = 0.7 * jax.random.normal(own_keys[2], (BATCH_ROWS, 1, HEAD_DIM), jnp.float32)
    v_cache = v_mean + jax.random.normal(own_keys[3], (BATCH_ROWS, CACHE_SIZE, HEAD_DIM), jnp.float32)
    cache_len = jax.random.randint(own_keys[4], (BATCH_ROWS,), 0, CACHE_SIZE, jnp.int32)
    cache_len = cache_len.at[0].set(CACHE_SIZE - 1)
    return {
        'hidden_in': hidden_in.astype(jnp.bfloat16),
        'k_cache': k_cache.astype(jnp.bfloat16),
        'v_cache': v_cache.astype(jnp.bfloat16),
        'cache_len': cache_len,
        'norm_attn': (0.3 * jax.random.normal(shared_keys[0], (D_MODEL,), jnp.float32)).astype(jnp.bfloat16),
        'norm_mlp': (0.3 * jax.random.normal(shared_keys[1], (D_MODEL,), jnp.float32)).astype(jnp.bfloat16),
        'w_q': scaled_normal(shared_keys[2], (D_MODEL, q_width), D_MODEL),
        'w_k': scaled_normal(shared_keys[3], (D_MODEL, HEAD_DIM), D_MODEL),
        'w_v': scaled_normal(shared_keys[4], (D_MODEL, HEAD_DIM), D_MODEL),
        'w_o': scaled_normal(shared_keys[5], (q_width, D_MODEL), q_width),
        'w_gate': scaled_normal(shared_keys[6], (D_MODEL, FF_DIM), D_MODEL),
        'w_up': scaled_normal(shared_keys[7], (D_MODEL, FF_DIM), D_MODEL),
        'w_down': scaled_normal(shared_keys[8], (FF_DIM, D_MODEL), FF_DIM),
    }


def rms_scale(values, gain_vec):
    wide_vals = values.astype(jnp.float32)
    inv_rms = lax.rsqrt(jnp.mean(wide_vals * wide_vals, axis=-1, keepdims=True) + 1e-6)
    return (wide_vals * inv_rms * (1.0 + gain_vec.astype(jnp.float32))).astype(jnp.bfloat16)


def rope_tables(positions, head_dim):
    half_dim = head_dim // 2
    inv_freq = 10000.0 ** (-2.0 * jnp.arange(half_dim, dtype=jnp.float32) / head_dim)
    angles = positions.astype(jnp.float32)[:, None] * inv_freq[None, :]
    return jnp.cos(angles), jnp.sin(angles)


def rotary(values, cos_t, sin_t):
    half_dim = values.shape[-1] // 2
    first_half = values[..., :half_dim]
    second_half = values[..., half_dim:]
    return jnp.concatenate([first_half * cos_t - second_half * sin_t, second_half * cos_t + first_half * sin_t], axis=-1)


def attend_row(row_args):
    q_row, k_row, v_row, k_hist, v_hist, position = row_args
    q_wide = q_row.astype(jnp.float32)
    hist_score = jnp.einsum('hd,td->ht', q_wide, k_hist.astype(jnp.float32))
    new_score = jnp.einsum('hd,d->h', q_wide, k_row.astype(jnp.float32))
    valid_mask = jnp.arange(k_hist.shape[0]) < position
    hist_score = jnp.where(valid_mask[None, :], hist_score, -jnp.inf)
    peak_score = jnp.maximum(jnp.max(hist_score, axis=-1), new_score)
    hist_weight = jnp.exp(hist_score - peak_score[:, None])
    new_weight = jnp.exp(new_score - peak_score)
    weight_sum = jnp.sum(hist_weight, axis=-1) + new_weight
    hist_prob = (hist_weight / weight_sum[:, None]).astype(jnp.bfloat16)
    new_prob = (new_weight / weight_sum).astype(jnp.bfloat16)
    attn_out = jnp.einsum('ht,td->hd', hist_prob.astype(jnp.float32), v_hist.astype(jnp.float32))
    attn_out = attn_out + new_prob.astype(jnp.float32)[:, None] * v_row.astype(jnp.float32)[None, :]
    return attn_out.astype(jnp.bfloat16)


def reference(hidden_in, k_cache, v_cache, cache_len, norm_attn, norm_mlp, w_q, w_k, w_v, w_o, w_gate, w_up, w_down):
    num_rows = hidden_in.shape[0]
    normed = rms_scale(hidden_in, norm_attn)
    q_lin = jnp.dot(normed, w_q, preferred_element_type=jnp.float32).reshape(num_rows, NUM_HEADS, HEAD_DIM)
    k_lin = jnp.dot(normed, w_k, preferred_element_type=jnp.float32)
    v_new = jnp.dot(normed, w_v, preferred_element_type=jnp.float32).astype(jnp.bfloat16)
    cos_t, sin_t = rope_tables(cache_len, HEAD_DIM)
    q_rot = (rotary(q_lin, cos_t[:, None, :], sin_t[:, None, :]) * HEAD_DIM ** -0.5).astype(jnp.bfloat16)
    k_new = rotary(k_lin, cos_t, sin_t).astype(jnp.bfloat16)
    attn_out = lax.map(attend_row, (q_rot, k_new, v_new, k_cache, v_cache, cache_len))
    mixed = jnp.dot(attn_out.reshape(num_rows, NUM_HEADS * HEAD_DIM), w_o, preferred_element_type=jnp.float32)
    x_mid = hidden_in.astype(jnp.float32) + mixed
    xn_mid = rms_scale(x_mid, norm_mlp)
    gate_act = jnp.dot(xn_mid, w_gate, preferred_element_type=jnp.float32)
    up_act = jnp.dot(xn_mid, w_up, preferred_element_type=jnp.float32)
    hidden_act = (jax.nn.gelu(gate_act, approximate=True) * up_act).astype(jnp.bfloat16)
    down_sum = jnp.dot(hidden_act, w_down, preferred_element_type=jnp.float32)
    hidden_out = (x_mid + down_sum).astype(jnp.bfloat16)
    return hidden_out, k_new, v_new
```

```python
import functools

import jax
import jax.numpy as jnp
from jax import lax
from jax.experimental import pallas as pl
from jax.experimental.pallas import tpu as pltpu
from jax.sharding import PartitionSpec as P

ROWS = 128
PIECE = 64
SUB = 32


def mlp_kernel(num_tp, xn_ref, xmid_ref, wg_hbm, wu_hbm, wd_hbm, out_ref,
               xg, hid, wg_buf, wu_buf, wd_buf, part, mate_out, mate_in, relay, from_x, from_y,
               wg_sem, wu_sem, wd_sem, send_sem, recv_sem):
    me = lax.axis_index('tp')
    mate = me + 1 - 2 * lax.rem(me, 2)
    xpeer = me + 2 - 4 * lax.rem(me // 2, 2)
    ypeer = me + 4 - 8 * (me // 4)

    h_tile = wg_buf.shape[2]
    n_tile = wd_buf.shape[2]
    h_steps = hid.shape[1] // h_tile
    n_steps = wd_hbm.shape[1] // n_tile
    groups = num_tp // 2
    gu_slots = wg_buf.shape[0]
    d_slots = wd_buf.shape[0]

    def gate_copy(step):
        cols = pl.ds(pl.multiple_of(lax.rem(step, h_steps) * h_tile, h_tile), h_tile)
        slot = lax.rem(step, gu_slots)
        return (pltpu.make_async_copy(wg_hbm.at[:, cols], wg_buf.at[slot], wg_sem.at[slot]),
                pltpu.make_async_copy(wu_hbm.at[:, cols], wu_buf.at[slot], wu_sem.at[slot]))

    def down_copy(step):
        cols = pl.ds(pl.multiple_of(lax.rem(step, n_steps) * n_tile, n_tile), n_tile)
        slot = lax.rem(step, d_slots)
        return pltpu.make_async_copy(wd_hbm.at[:, cols], wd_buf.at[slot], wd_sem.at[slot])

    for step in range(gu_slots):
        for copy in gate_copy(jnp.int32(step)):
            copy.start()
    for step in range(d_slots):
        down_copy(jnp.int32(step)).start()

    barrier = pltpu.get_barrier_semaphore()
    for peer in (mate, xpeer, ypeer):
        pl.semaphore_signal(barrier, inc=1, device_id={'tp': peer}, device_id_type=pl.DeviceIdType.MESH)
    pl.semaphore_wait(barrier, 3)

    count = [0]

    def remote(src, dst, peer):
        k = count[0]
        count[0] += 1
        return pltpu.make_async_remote_copy(
            src_ref=src, dst_ref=dst, send_sem=send_sem.at[k], recv_sem=recv_sem.at[k],
            device_id={'tp': peer}, device_id_type=pl.DeviceIdType.MESH)

    def rows_of(start, size):
        return xg.at[pl.ds(start, size), :]

    top, bot = xn_ref.at[pl.ds(0, PIECE), :], xn_ref.at[pl.ds(PIECE, PIECE), :]
    own_mate = remote(xn_ref, rows_of(128, 128), mate)
    near_x = remote(top, rows_of(256, 64), xpeer)
    near_y = remote(bot, rows_of(320, 64), ypeer)
    diag_y = remote(rows_of(256, 64), rows_of(512, 64), ypeer)
    diag_x = remote(rows_of(320, 64), rows_of(576, 64), xpeer)
    far_x = remote(bot, rows_of(768, 64), xpeer)
    far_y = remote(top, rows_of(832, 64), ypeer)
    near_mate = remote(rows_of(256, 128), rows_of(384, 128), mate)
    diag_mate = remote(rows_of(512, 128), rows_of(640, 128), mate)
    far_mate = remote(rows_of(768, 128), rows_of(896, 128), mate)
    pair_sum = [remote(mate_out.at[g % 2], mate_in.at[g], mate) for g in range(groups)]
    chunks = range(PIECE // SUB)

    def span(lead, c):
        return pl.ds(lead + c * SUB, SUB)

    near_sx = [remote(part.at[1, span(0, c), :], from_x.at[span(0, c), :], xpeer) for c in chunks]
    near_sy = [remote(part.at[1, span(PIECE, c), :], from_y.at[span(PIECE, c), :], ypeer) for c in chunks]
    diag_sx = [remote(part.at[2, span(0, c), :], relay.at[span(PIECE, c), :], xpeer) for c in chunks]
    diag_sy = [remote(part.at[2, span(PIECE, c), :], relay.at[span(0, c), :], ypeer) for c in chunks]
    far_sx = [remote(part.at[3, span(0, c), :], from_x.at[span(PIECE, c), :], xpeer) for c in chunks]
    far_sy = [remote(part.at[3, span(PIECE, c), :], from_y.at[span(0, c), :], ypeer) for c in chunks]

    near_x.start()
    near_y.start()
    own_mate.start()
    xg[pl.ds(0, ROWS), :] = xn_ref[...]
    own_mate.wait_recv()

    def add_pair(g, after=None):
        @pl.loop(0, ROWS // 8)
        def _(r):
            rows = pl.ds(pl.multiple_of(r * 8, 8), 8)
            part[g, rows, :] += mate_in[g, rows, :]

    def hook(g, where, action):
        return (g, where, action)

    def gather_near():
        near_x.wait_recv()
        diag_y.start()
        near_y.wait_recv()
        diag_x.start()
        far_x.start()
        far_y.start()
        near_mate.start()

    def gather_diag():
        diag_y.wait_recv()
        diag_x.wait_recv()
        diag_mate.start()

    def gather_far():
        far_x.wait_recv()
        far_y.wait_recv()
        far_mate.start()

    def sum_own():
        pair_sum[0].wait_recv()
        add_pair(0)

    def send_near():
        pair_sum[1].wait_recv()
        add_pair(1)
        for c in chunks:
            near_sx[c].start()
            near_sy[c].start()

    def send_diag():
        pair_sum[2].wait_recv()
        add_pair(2)
        for c in chunks:
            diag_sx[c].start()
            diag_sy[c].start()

    before_h = {
        (1, 0): near_mate.wait_recv,
        (1, h_steps // 2): sum_own,
        (2, 0): diag_mate.wait_recv,
        (2, h_steps // 2): send_near,
        (3, 0): far_mate.wait_recv,
        (3, h_steps // 2): send_diag,
    }
    before_n = {
        (0, 0): gather_near,
        (1, 0): gather_diag,
        (2, 0): gather_far,
        (2, 1): pair_sum[0].wait_send,
        (3, 0): pair_sum[1].wait_send,
    }
    before_n[(2, 0)] = lambda: (gather_far(), pair_sum[0].wait_send())
    del before_n[(2, 1)]

    def run_hooks(table, g, step):
        for (hg, hs), action in table.items():
            @pl.when(jnp.logical_and(g == hg, step == hs))
            def _():
                action()

    @pl.loop(0, groups)
    def _(g):
        rows = pl.ds(pl.multiple_of(g * (2 * ROWS), 2 * ROWS), 2 * ROWS)

        @pl.loop(0, h_steps)
        def _(j):
            run_hooks(before_h, g, j)
            step = g * h_steps + j
            slot = lax.rem(step, gu_slots)
            for copy in gate_copy(step):
                copy.wait()
            gate_act = jnp.dot(xg[rows, :], wg_buf[slot], preferred_element_type=jnp.float32)
            up_act = jnp.dot(xg[rows, :], wu_buf[slot], preferred_element_type=jnp.float32)
            cols = pl.ds(pl.multiple_of(j * h_tile, h_tile), h_tile)
            hid[:, cols] = (jax.nn.gelu(gate_act, approximate=True) * up_act).astype(jnp.bfloat16)

            @pl.when(step + gu_slots < groups * h_steps)
            def _():
                for copy in gate_copy(step + gu_slots):
                    copy.start()

        @pl.loop(0, n_steps)
        def _(n):
            run_hooks(before_n, g, n)
            step = g * n_steps + n
            slot = lax.rem(step, d_slots)
            down_copy(step).wait()
            res = jnp.dot(hid[...], wd_buf[slot], preferred_element_type=jnp.float32)
            cols = pl.ds(pl.multiple_of(n * n_tile, n_tile), n_tile)
            part[g, :, cols] = res[:ROWS]
            mate_out[lax.rem(g, 2), :, cols] = res[ROWS:]

            @pl.when(step + d_slots < groups * n_steps)
            def _():
                down_copy(step + d_slots).start()

        for hg in range(groups):
            @pl.when(g == hg)
            def _():
                pair_sum[hg].start()

    pair_sum[3].wait_recv()
    add_pair(3)
    for c in chunks:
        diag_sy[c].wait_recv()
        part[3, pl.ds(c * SUB, SUB), :] += relay[pl.ds(c * SUB, SUB), :]
        far_sx[c].start()
        diag_sx[c].wait_recv()
        part[3, pl.ds(PIECE + c * SUB, SUB), :] += relay[pl.ds(PIECE + c * SUB, SUB), :]
        far_sy[c].start()
    for c in chunks:
        near_sx[c].wait_recv()
        near_sy[c].wait_recv()
    part[0] = part[0] + xmid_ref[...]
    part[0, pl.ds(0, PIECE), :] += from_x[pl.ds(0, PIECE), :]
    part[0, pl.ds(PIECE, PIECE), :] += from_y[pl.ds(PIECE, PIECE), :]
    for c in chunks:
        low, high = pl.ds(c * SUB, SUB), pl.ds(PIECE + c * SUB, SUB)
        far_sx[c].wait_recv()
        out_ref[high, :] = (part[0, high, :] + from_x[high, :]).astype(out_ref.dtype)
        far_sy[c].wait_recv()
        out_ref[low, :] = (part[0, low, :] + from_y[low, :]).astype(out_ref.dtype)
    for copy in ([own_mate, near_x, near_y, diag_y, diag_x, far_x, far_y, near_mate, diag_mate, far_mate]
                 + pair_sum[2:] + near_sx + near_sy + diag_sx + diag_sy + far_sx + far_sy):
        copy.wait_send()


def exchange_mlp(num_tp, xn_mid, x_mid, w_gate, w_up, w_down):
    width = xn_mid.shape[1]
    hidden = w_gate.shape[1]
    h_tile, n_tile = 256, 512
    gu_slots, d_slots = 3, 3
    groups = num_tp // 2
    copies = 10 + groups + 6 * (PIECE // SUB)
    f32, bf16 = jnp.float32, jnp.bfloat16
    vmem = pl.BlockSpec(memory_space=pltpu.VMEM)
    hbm = pl.BlockSpec(memory_space=pl.ANY)
    return pl.pallas_call(
        functools.partial(mlp_kernel, num_tp),
        out_shape=jax.ShapeDtypeStruct((ROWS, width), bf16),
        in_specs=[vmem, vmem, hbm, hbm, hbm],
        out_specs=vmem,
        scratch_shapes=[
            pltpu.VMEM((num_tp * ROWS, width), bf16),
            pltpu.VMEM((2 * ROWS, hidden), bf16),
            pltpu.VMEM((gu_slots, width, h_tile), bf16),
            pltpu.VMEM((gu_slots, width, h_tile), bf16),
            pltpu.VMEM((d_slots, hidden, n_tile), bf16),
            pltpu.VMEM((groups, ROWS, width), f32),
            pltpu.VMEM((2, ROWS, width), f32),
            pltpu.VMEM((groups, ROWS, width), f32),
            pltpu.VMEM((ROWS, width), f32),
            pltpu.VMEM((ROWS, width), f32),
            pltpu.VMEM((ROWS, width), f32),
            pltpu.SemaphoreType.DMA((gu_slots,)),
            pltpu.SemaphoreType.DMA((gu_slots,)),
            pltpu.SemaphoreType.DMA((d_slots,)),
            pltpu.SemaphoreType.DMA((copies,)),
            pltpu.SemaphoreType.DMA((copies,)),
        ],
        compiler_params=pltpu.CompilerParams(
            collective_id=0, has_side_effects=True, vmem_limit_bytes=67043328),
        cost_estimate=pl.CostEstimate(flops=6 * num_tp * ROWS * width * hidden,
                                      bytes_accessed=6 * width * hidden * groups, transcendentals=0),
        name='exchange_mlp',
    )(xn_mid, x_mid, w_gate, w_up, w_down)


def rms_scale(values, gain_vec):
    wide_vals = values.astype(jnp.float32)
    inv_rms = lax.rsqrt(jnp.mean(wide_vals * wide_vals, axis=-1, keepdims=True) + 1e-6)
    return (wide_vals * inv_rms * (1.0 + gain_vec.astype(jnp.float32))).astype(jnp.bfloat16)


def rope_tables(positions, head_dim):
    half_dim = head_dim // 2
    inv_freq = 10000.0 ** (-2.0 * jnp.arange(half_dim, dtype=jnp.float32) / head_dim)
    angles = positions.astype(jnp.float32)[:, None] * inv_freq[None, :]
    return jnp.cos(angles), jnp.sin(angles)


def rotary(values, cos_t, sin_t):
    half_dim = values.shape[-1] // 2
    first_half = values[..., :half_dim]
    second_half = values[..., half_dim:]
    return jnp.concatenate([first_half * cos_t - second_half * sin_t, second_half * cos_t + first_half * sin_t], axis=-1)


def attend(q_rot, k_new, v_new, k_cache, v_cache, cache_len):
    hist_score = jnp.einsum('bhd,btd->bht', q_rot, k_cache, preferred_element_type=jnp.float32)
    new_score = jnp.einsum('bhd,bd->bh', q_rot, k_new, preferred_element_type=jnp.float32)
    valid_mask = lax.broadcasted_iota(jnp.int32, (1, 1, k_cache.shape[1]), 2) < cache_len[:, None, None]
    hist_score = jnp.where(valid_mask, hist_score, -jnp.inf)
    peak_score = jnp.maximum(jnp.max(hist_score, axis=-1), new_score)
    hist_weight = jnp.exp(hist_score - peak_score[..., None])
    new_weight = jnp.exp(new_score - peak_score)
    weight_sum = jnp.sum(hist_weight, axis=-1) + new_weight
    hist_prob = (hist_weight / weight_sum[..., None]).astype(jnp.bfloat16)
    new_prob = (new_weight / weight_sum).astype(jnp.bfloat16)
    attn_out = jnp.einsum('bht,btd->bhd', hist_prob, v_cache, preferred_element_type=jnp.float32)
    attn_out = attn_out + new_prob.astype(jnp.float32)[..., None] * v_new.astype(jnp.float32)[:, None, :]
    return attn_out.astype(jnp.bfloat16)


def attention_block(hidden_in, k_cache, v_cache, cache_len, norm_attn, w_q, w_k, w_v, w_o):
    num_rows = hidden_in.shape[0]
    head_dim = w_k.shape[1]
    num_heads = w_q.shape[1] // head_dim
    normed = rms_scale(hidden_in, norm_attn)
    q_lin = jnp.dot(normed, w_q, preferred_element_type=jnp.float32).reshape(num_rows, num_heads, head_dim)
    k_lin = jnp.dot(normed, w_k, preferred_element_type=jnp.float32)
    v_new = jnp.dot(normed, w_v, preferred_element_type=jnp.float32).astype(jnp.bfloat16)
    cos_t, sin_t = rope_tables(cache_len, head_dim)
    q_rot = (rotary(q_lin, cos_t[:, None, :], sin_t[:, None, :]) * head_dim ** -0.5).astype(jnp.bfloat16)
    k_new = rotary(k_lin, cos_t, sin_t).astype(jnp.bfloat16)
    attn_out = attend(q_rot, k_new, v_new, k_cache, v_cache, cache_len)
    mixed = jnp.dot(attn_out.reshape(num_rows, num_heads * head_dim), w_o, preferred_element_type=jnp.float32)
    return hidden_in.astype(jnp.float32) + mixed, k_new, v_new


def solution(mesh):
    row_spec = P(('dp', 'tp'), None)
    cache_spec = P(('dp', 'tp'), None, None)
    full_vec = P(None)
    full_mat = P(None, None)

    def per_device(hidden_in, k_cache, v_cache, cache_len, norm_attn, norm_mlp, w_q, w_k, w_v, w_o, w_gate, w_up, w_down):
        x_mid, k_new, v_new = attention_block(hidden_in, k_cache, v_cache, cache_len, norm_attn, w_q, w_k, w_v, w_o)
        xn_mid = rms_scale(x_mid, norm_mlp)
        hidden_out = exchange_mlp(mesh.shape['tp'], xn_mid, x_mid, w_gate, w_up, w_down)
        return hidden_out, k_new, v_new

    return jax.shard_map(
        per_device,
        mesh=mesh,
        in_specs=(row_spec, cache_spec, cache_spec, P(('dp', 'tp')), full_vec, full_vec,
                  full_mat, full_mat, full_mat, full_mat, P(None, 'tp'), P(None, 'tp'), P('tp', None)),
        out_specs=(row_spec, row_spec, row_spec),
        check_vma=False,
    )
```

```python
import functools

import jax
import jax.numpy as jnp
from jax import lax
from jax.experimental import pallas as pl
from jax.experimental.pallas import tpu as pltpu
from jax.sharding import PartitionSpec as P

ROWS = 128
PIECE = 64
SUB = 32


def mlp_kernel(num_tp, xn_ref, xmid_ref, wg_hbm, wu_hbm, wd_hbm, out_ref,
               xg, hid, wg_buf, wu_buf, wd_buf, part, mate_out, mate_in, relay, from_x, from_y,
               wg_sem, wu_sem, wd_sem, send_sem, recv_sem):
    me = lax.axis_index('tp')
    mate = me + 1 - 2 * lax.rem(me, 2)
    xpeer = me + 2 - 4 * lax.rem(me // 2, 2)
    ypeer = me + 4 - 8 * (me // 4)

    h_tile = wg_buf.shape[2]
    n_tile = wd_buf.shape[2]
    h_steps = hid.shape[2] // h_tile
    n_steps = wd_hbm.shape[1] // n_tile
    groups = num_tp // 2
    gu_slots = wg_buf.shape[0]
    d_slots = wd_buf.shape[0]

    def gate_copy(step):
        cols = pl.ds(pl.multiple_of(lax.rem(step, h_steps) * h_tile, h_tile), h_tile)
        slot = lax.rem(step, gu_slots)
        return (pltpu.make_async_copy(wg_hbm.at[:, cols], wg_buf.at[slot], wg_sem.at[slot]),
                pltpu.make_async_copy(wu_hbm.at[:, cols], wu_buf.at[slot], wu_sem.at[slot]))

    def down_copy(step):
        cols = pl.ds(pl.multiple_of(lax.rem(step, n_steps) * n_tile, n_tile), n_tile)
        slot = lax.rem(step, d_slots)
        return pltpu.make_async_copy(wd_hbm.at[:, cols], wd_buf.at[slot], wd_sem.at[slot])

    for step in range(gu_slots):
        for copy in gate_copy(jnp.int32(step)):
            copy.start()
    for step in range(d_slots):
        down_copy(jnp.int32(step)).start()

    barrier = pltpu.get_barrier_semaphore()
    for peer in (mate, xpeer, ypeer):
        pl.semaphore_signal(barrier, inc=1, device_id={'tp': peer}, device_id_type=pl.DeviceIdType.MESH)
    pl.semaphore_wait(barrier, 3)

    count = [0]

    def remote(src, dst, peer):
        k = count[0]
        count[0] += 1
        return pltpu.make_async_remote_copy(
            src_ref=src, dst_ref=dst, send_sem=send_sem.at[k], recv_sem=recv_sem.at[k],
            device_id={'tp': peer}, device_id_type=pl.DeviceIdType.MESH)

    def rows_of(start, size):
        return xg.at[pl.ds(start, size), :]

    top, bot = xn_ref.at[pl.ds(0, PIECE), :], xn_ref.at[pl.ds(PIECE, PIECE), :]
    chunks = range(PIECE // SUB)

    def span(lead, c):
        return pl.ds(lead + c * SUB, SUB)

    own_mate = remote(xn_ref, rows_of(128, 128), mate)
    near_x = remote(top, rows_of(256, 64), xpeer)
    near_y = remote(bot, rows_of(320, 64), ypeer)
    diag_y = remote(rows_of(256, 64), rows_of(512, 64), ypeer)
    diag_x = remote(rows_of(320, 64), rows_of(576, 64), xpeer)
    far_x = [remote(xn_ref.at[span(PIECE, c), :], xg.at[span(768, c), :], xpeer) for c in chunks]
    far_y = [remote(xn_ref.at[span(0, c), :], xg.at[span(832, c), :], ypeer) for c in chunks]
    near_mate = remote(rows_of(256, 128), rows_of(384, 128), mate)
    diag_mate = remote(rows_of(512, 128), rows_of(640, 128), mate)
    far_mate = remote(rows_of(768, 128), rows_of(896, 128), mate)
    width = xn_ref.shape[1]
    quarters = 4
    side = [pl.ds(i * (width // quarters), width // quarters) for i in range(quarters)]
    pair = [[remote(mate_out.at[(g + 1) % 2, :, cols], mate_in.at[g, :, cols], mate) for cols in side]
            for g in range(groups)]
    near_sx = [remote(part.at[1, span(0, c), :], from_x.at[span(0, c), :], xpeer) for c in chunks]
    near_sy = [remote(part.at[1, span(PIECE, c), :], from_y.at[span(PIECE, c), :], ypeer) for c in chunks]
    diag_sx = [remote(part.at[2, span(0, c), :], relay.at[span(PIECE, c), :], xpeer) for c in chunks]
    diag_sy = [remote(part.at[2, span(PIECE, c), :], relay.at[span(0, c), :], ypeer) for c in chunks]
    far_sx = [remote(part.at[3, span(0, c), :], from_x.at[span(PIECE, c), :], xpeer) for c in chunks]
    far_sy = [remote(part.at[3, span(PIECE, c), :], from_y.at[span(0, c), :], ypeer) for c in chunks]

    near_x.start()
    near_y.start()
    far_x[0].start()
    far_y[0].start()
    own_mate.start()
    xg[pl.ds(0, ROWS), :] = xn_ref[...]
    own_mate.wait_recv()

    def add_pair(g):
        for copy in pair[g]:
            copy.wait_recv()

        @pl.loop(0, ROWS // 8)
        def _(r):
            rows = pl.ds(pl.multiple_of(r * 8, 8), 8)
            part[g, rows, :] += mate_in[g, rows, :]

    def gather_near():
        near_x.wait_recv()
        diag_y.start()
        near_y.wait_recv()
        diag_x.start()
        far_x[1].start()
        far_y[1].start()
        near_mate.start()

    def gather_diag():
        diag_y.wait_recv()
        diag_x.wait_recv()
        diag_mate.start()

    def gather_far():
        for c in chunks:
            far_x[c].wait_recv()
            far_y[c].wait_recv()
        far_mate.start()

    def send_near():
        add_pair(1)
        for c in chunks:
            near_sx[c].start()
            near_sy[c].start()

    def send_diag():
        add_pair(2)
        for c in chunks:
            diag_sx[c].start()
            diag_sy[c].start()

    def free_slot(g):
        for copy in pair[g]:
            copy.wait_send()

    def start_diag():
        send_near()
        gather_diag()
        diag_mate.wait_recv()

    def start_far():
        send_diag()
        far_mate.wait_recv()

    def pass_on(c):
        diag_sy[c].wait_recv()
        part[3, span(0, c), :] += relay[span(0, c), :]
        far_sx[c].start()
        diag_sx[c].wait_recv()
        part[3, span(PIECE, c), :] += relay[span(PIECE, c), :]
        far_sy[c].start()

    before_h = {
        (0, h_steps - 1): gather_near,
        (1, 0): near_mate.wait_recv,
        (2, 0): start_diag,
        (2, h_steps - 1): gather_far,
        (3, 0): start_far,
    }
    before_n = {
        (3, 0): lambda: free_slot(1),
        (0, 0): lambda: free_slot(2),
        (0, n_steps // 2): lambda: add_pair(3),
        (0, n_steps - 2): lambda: pass_on(0),
    }

    def run_hooks(table, g, step):
        for (hg, hs), action in table.items():
            @pl.when(jnp.logical_and(g == hg, step == hs))
            def _():
                action()

    @pl.loop(0, groups + 1)
    def _(turn):
        @pl.when(turn < groups)
        def _():
            rows = pl.ds(pl.multiple_of(turn * (2 * ROWS), 2 * ROWS), 2 * ROWS)
            keep = jnp.minimum(turn, 1)

            @pl.loop(0, h_steps)
            def _(j):
                run_hooks(before_h, turn, j)
                step = turn * h_steps + j
                slot = lax.rem(step, gu_slots)
                for copy in gate_copy(step):
                    copy.wait()
                gate_act = jnp.dot(xg[rows, :], wg_buf[slot], preferred_element_type=jnp.float32)
                up_act = jnp.dot(xg[rows, :], wu_buf[slot], preferred_element_type=jnp.float32)
                cols = pl.ds(pl.multiple_of(j * h_tile, h_tile), h_tile)
                hid[keep, :, cols] = (jax.nn.gelu(gate_act, approximate=True) * up_act).astype(jnp.bfloat16)

                @pl.when(step + gu_slots < groups * h_steps)
                def _():
                    for copy in gate_copy(step + gu_slots):
                        copy.start()

        @pl.when(turn > 0)
        def _():
            g = lax.rem(turn, groups)
            keep = jnp.minimum(g, 1)

            @pl.loop(0, n_steps)
            def _(n):
                run_hooks(before_n, g, n)
                step = (turn - 1) * n_steps + n
                slot = lax.rem(step, d_slots)
                down_copy(step).wait()
                res = jnp.dot(hid[keep], wd_buf[slot], preferred_element_type=jnp.float32)
                cols = pl.ds(pl.multiple_of(n * n_tile, n_tile), n_tile)
                part[g, :, cols] = res[:ROWS]
                mate_out[lax.rem(g + 1, 2), :, cols] = res[ROWS:]

                for hg in range(groups):
                    for i in range(quarters):
                        @pl.when(jnp.logical_and(g == hg, n == (i + 1) * n_steps // quarters - 1))
                        def _():
                            pair[hg][i].start()

                @pl.when(step + d_slots < groups * n_steps)
                def _():
                    down_copy(step + d_slots).start()


    add_pair(0)
    for c in chunks:
        near_sx[c].wait_recv()
        near_sy[c].wait_recv()
    part[0] = part[0] + xmid_ref[...]
    part[0, pl.ds(0, PIECE), :] += from_x[pl.ds(0, PIECE), :]
    part[0, pl.ds(PIECE, PIECE), :] += from_y[pl.ds(PIECE, PIECE), :]
    for c in chunks[1:]:
        pass_on(c)
    for c in chunks:
        low, high = span(0, c), span(PIECE, c)
        far_sx[c].wait_recv()
        out_ref[high, :] = (part[0, high, :] + from_x[high, :]).astype(out_ref.dtype)
        far_sy[c].wait_recv()
        out_ref[low, :] = (part[0, low, :] + from_y[low, :]).astype(out_ref.dtype)
    for copy in ([own_mate, near_x, near_y, diag_y, diag_x, near_mate, diag_mate, far_mate]
                 + far_x + far_y + pair[3] + pair[0]
                 + near_sx + near_sy + diag_sx + diag_sy + far_sx + far_sy):
        copy.wait_send()


def exchange_mlp(num_tp, xn_mid, x_mid, w_gate, w_up, w_down):
    width = xn_mid.shape[1]
    hidden = w_gate.shape[1]
    h_tile, n_tile = 256, 512
    gu_slots, d_slots = 3, 3
    groups = num_tp // 2
    copies = 8 + 4 * groups + 8 * (PIECE // SUB)
    f32, bf16 = jnp.float32, jnp.bfloat16
    vmem = pl.BlockSpec(memory_space=pltpu.VMEM)
    hbm = pl.BlockSpec(memory_space=pl.ANY)
    return pl.pallas_call(
        functools.partial(mlp_kernel, num_tp),
        out_shape=jax.ShapeDtypeStruct((ROWS, width), bf16),
        in_specs=[vmem, vmem, hbm, hbm, hbm],
        out_specs=vmem,
        scratch_shapes=[
            pltpu.VMEM((num_tp * ROWS, width), bf16),
            pltpu.VMEM((2, 2 * ROWS, hidden), bf16),
            pltpu.VMEM((gu_slots, width, h_tile), bf16),
            pltpu.VMEM((gu_slots, width, h_tile), bf16),
            pltpu.VMEM((d_slots, hidden, n_tile), bf16),
            pltpu.VMEM((groups, ROWS, width), f32),
            pltpu.VMEM((2, ROWS, width), f32),
            pltpu.VMEM((groups, ROWS, width), f32),
            pltpu.VMEM((ROWS, width), f32),
            pltpu.VMEM((ROWS, width), f32),
            pltpu.VMEM((ROWS, width), f32),
            pltpu.SemaphoreType.DMA((gu_slots,)),
            pltpu.SemaphoreType.DMA((gu_slots,)),
            pltpu.SemaphoreType.DMA((d_slots,)),
            pltpu.SemaphoreType.DMA((copies,)),
            pltpu.SemaphoreType.DMA((copies,)),
        ],
        compiler_params=pltpu.CompilerParams(
            collective_id=0, has_side_effects=True, vmem_limit_bytes=67043328),
        cost_estimate=pl.CostEstimate(flops=6 * num_tp * ROWS * width * hidden,
                                      bytes_accessed=6 * width * hidden * groups, transcendentals=0),
        name='exchange_mlp',
    )(xn_mid, x_mid, w_gate, w_up, w_down)


def rope_tables(positions, head_dim):
    half_dim = head_dim // 2
    inv_freq = 10000.0 ** (-2.0 * jnp.arange(half_dim, dtype=jnp.float32) / head_dim)
    angles = positions.astype(jnp.float32)[:, None] * inv_freq[None, :]
    return jnp.cos(angles), jnp.sin(angles)


TEAM = 8
BLOCK = 128
AHEAD = 4


def attention_kernel(order, lens, hid_ref, ga_ref, gm_ref, cos_ref, sin_ref, wk_hbm, wv_hbm, wq_hbm, wo_hbm,
                     kc_hbm, vc_hbm, xn_out, xmid_out, knew_out, vnew_out,
                     w_buf, k_buf, v_buf, xn, q_lo, q_hi, o_lo, o_hi, k_row, v_row, squares,
                     w_sem, k_sem, v_sem):
    num_rows, width = hid_ref.shape
    head_dim = wk_hbm.shape[1]
    half = head_dim // 2
    heads = wq_hbm.shape[1] // head_dim
    tiles = wo_hbm.shape[1] // head_dim
    teams = num_rows // TEAM
    slots = k_buf.shape[0]
    w_slots = w_buf.shape[0]
    max_units = kc_hbm.shape[1] // BLOCK
    f32, bf16 = jnp.float32, jnp.bfloat16

    def tile_copy(src, tile, slot):
        cols = pl.ds(pl.multiple_of(tile * head_dim, head_dim), head_dim)
        return pltpu.make_async_copy(src.at[:, cols], w_buf.at[slot], w_sem.at[slot])

    def head_copy(head):
        return tile_copy(wq_hbm, head, lax.rem(head + 2, w_slots))

    def out_copy(tile):
        return tile_copy(wo_hbm, tile, tile)

    def units_of(team):
        longest = lens[order[team * TEAM + TEAM - 1]]
        return jnp.maximum((longest + BLOCK - 1) // BLOCK, 1)

    def key_copy(team, r, n):
        slot, span = lax.rem(team, slots), pl.ds(0, n * BLOCK)
        return pltpu.make_async_copy(kc_hbm.at[order[team * TEAM + r], span, :],
                                     k_buf.at[slot, r, span, :], k_sem.at[slot, r])

    def value_copy(team, r, n):
        slot, span = lax.rem(team, slots), pl.ds(0, n * BLOCK)
        return pltpu.make_async_copy(vc_hbm.at[order[team * TEAM + r], span, :],
                                     v_buf.at[slot, r, span, :], v_sem.at[slot, r])

    def fetch(team):
        units = units_of(team)
        for n in range(1, max_units + 1):
            @pl.when(units == n)
            def _():
                for r in range(TEAM):
                    key_copy(team, r, n).start()
                    value_copy(team, r, n).start()

    def normalise(src, gain_ref, dst):
        gain = 1.0 + gain_ref[...].astype(f32)[None, :]

        @pl.loop(0, num_rows // 16)
        def _(i):
            rows = pl.ds(pl.multiple_of(i * 16, 16), 16)
            wide = src[rows, :].astype(f32)
            inv = lax.rsqrt(jnp.mean(wide * wide, axis=-1, keepdims=True) + 1e-6)
            dst[rows, :] = (wide * inv * gain).astype(bf16)

    first = [tile_copy(wk_hbm, 0, 0), tile_copy(wv_hbm, 0, 1)]
    for copy in first:
        copy.start()
    for head in range(AHEAD - 2):
        head_copy(jnp.int32(head)).start()
    normalise(hid_ref, ga_ref, xn)

    def rotate(lin):
        low, high = lin[:, :half], lin[:, half:]
        cos_t, sin_t = cos_ref[...], sin_ref[...]
        return low * cos_t - high * sin_t, high * cos_t + low * sin_t

    first[0].wait()
    head_copy(jnp.int32(AHEAD - 2)).start()
    low, high = rotate(jnp.dot(xn[...], w_buf[0], preferred_element_type=f32))
    key = jnp.concatenate([low, high], axis=-1).astype(bf16)
    knew_out[...] = key
    k_row[...] = key.astype(f32)
    first[1].wait()
    head_copy(jnp.int32(AHEAD - 1)).start()
    value = jnp.dot(xn[...], w_buf[1], preferred_element_type=f32).astype(bf16)
    vnew_out[...] = value
    v_row[...] = value.astype(f32)

    early = range(slots - 1)

    @pl.loop(0, heads)
    def _(head):
        head_copy(head).wait()

        @pl.when(head + AHEAD < heads)
        def _():
            head_copy(head + AHEAD).start()
        for team in early:
            @pl.when(head == heads - AHEAD + team)
            def _():
                fetch(jnp.int32(team))
        low, high = rotate(jnp.dot(xn[...], w_buf[lax.rem(head + 2, w_slots)], preferred_element_type=f32))
        spots = pl.ds(head, num_rows, stride=heads)
        q_lo[spots, :] = (low * head_dim ** -0.5).astype(bf16).astype(f32)
        q_hi[spots, :] = (high * head_dim ** -0.5).astype(bf16).astype(f32)

    def attend(team, n):
        slot = lax.rem(team, slots)
        size = n * BLOCK
        rows = [order[team * TEAM + r] for r in range(TEAM)]
        spans = [pl.ds(pl.multiple_of(row * heads, heads), heads) for row in rows]
        for r in range(TEAM):
            key_copy(team, r, n).wait()
        wide = [jnp.concatenate([q_lo[span, :], q_hi[span, :]], axis=-1) for span in spans]
        scores = [lax.dot_general(wide[r].astype(bf16), k_buf[slot, r, pl.ds(0, size), :], (((1,), (1,)), ((), ())),
                                  preferred_element_type=f32) for r in range(TEAM)]
        for r in range(TEAM):
            value_copy(team, r, n).wait()
        place = lax.broadcasted_iota(jnp.int32, scores[0].shape, 1)
        probs, news = [], []
        for r in range(TEAM):
            score = jnp.where(place < lens[rows[r]], scores[r], -jnp.inf)
            fresh = jnp.sum(wide[r] * k_row[pl.ds(rows[r], 1), :], axis=-1, keepdims=True)
            peak = jnp.maximum(jnp.max(score, axis=-1, keepdims=True), fresh)
            weight = jnp.exp(score - peak)
            fresh = jnp.exp(fresh - peak)
            scale = 1.0 / (jnp.sum(weight, axis=-1, keepdims=True) + fresh)
            probs.append((weight * scale).astype(bf16))
            news.append((fresh * scale).astype(bf16).astype(f32))
        for r in range(TEAM):
            mixed = jnp.dot(probs[r], v_buf[slot, r, pl.ds(0, size), :], preferred_element_type=f32)
            mixed = mixed + news[r] * v_row[pl.ds(rows[r], 1), :]
            mixed = mixed.astype(bf16).astype(f32)
            o_lo[spans[r], :] = mixed[:, :half]
            o_hi[spans[r], :] = mixed[:, half:]

    share = tiles // teams

    @pl.loop(0, teams)
    def _(team):
        @pl.when(team + slots - 1 < teams)
        def _():
            fetch(team + slots - 1)
        for part in range(share):
            out_copy(team * share + part).start()
        units = units_of(team)
        for n in range(1, max_units + 1):
            @pl.when(units == n)
            def _():
                attend(team, n)

    for head in range(heads):
        spots = pl.ds(head, num_rows, stride=heads)
        xn[:, pl.ds(head * head_dim, half)] = o_lo[spots, :].astype(bf16)
        xn[:, pl.ds(head * head_dim + half, half)] = o_hi[spots, :].astype(bf16)
    squares[...] = jnp.zeros_like(squares)

    @pl.loop(0, tiles)
    def _(tile):
        out_copy(tile).wait()
        cols = pl.ds(pl.multiple_of(tile * head_dim, head_dim), head_dim)
        mixed = hid_ref[:, cols].astype(f32) + jnp.dot(xn[...], w_buf[tile], preferred_element_type=f32)
        xmid_out[:, cols] = mixed
        mixed = mixed * mixed
        squares[...] += mixed[:, :half] + mixed[:, half:]

    gain = 1.0 + gm_ref[...].astype(f32)[None, :]

    @pl.loop(0, num_rows // 16)
    def _(i):
        rows = pl.ds(pl.multiple_of(i * 16, 16), 16)
        inv = lax.rsqrt(jnp.sum(squares[rows, :], axis=-1, keepdims=True) * (1.0 / width) + 1e-6)
        xn_out[rows, :] = (xmid_out[rows, :] * inv * gain).astype(bf16)


def attention_block(hidden_in, k_cache, v_cache, cache_len, norm_attn, norm_mlp, w_q, w_k, w_v, w_o):
    num_rows, width = hidden_in.shape
    head_dim = w_k.shape[1]
    half = head_dim // 2
    heads = w_q.shape[1] // head_dim
    cos_t, sin_t = rope_tables(cache_len, head_dim)
    spot = jnp.arange(num_rows, dtype=jnp.int32)
    ahead = (cache_len[None, :] < cache_len[:, None]) | (
        (cache_len[None, :] == cache_len[:, None]) & (spot[None, :] < spot[:, None]))
    rank = jnp.sum(ahead.astype(jnp.int32), axis=1)
    order = jnp.sum(jnp.where(rank[:, None] == spot[None, :], spot[:, None], 0), axis=0)
    slots, w_slots = 3, w_o.shape[1] // head_dim
    f32, bf16 = jnp.float32, jnp.bfloat16
    vmem = pl.BlockSpec(memory_space=pltpu.VMEM)
    smem = pl.BlockSpec(memory_space=pltpu.SMEM)
    hbm = pl.BlockSpec(memory_space=pl.ANY)
    team_shape = (slots, TEAM, k_cache.shape[1], head_dim)
    return pl.pallas_call(
        attention_kernel,
        out_shape=[jax.ShapeDtypeStruct((num_rows, width), bf16), jax.ShapeDtypeStruct((num_rows, width), f32),
                   jax.ShapeDtypeStruct((num_rows, head_dim), bf16), jax.ShapeDtypeStruct((num_rows, head_dim), bf16)],
        in_specs=[smem, smem, vmem, vmem, vmem, vmem, vmem, hbm, hbm, hbm, hbm, hbm, hbm],
        out_specs=[vmem] * 4,
        scratch_shapes=[
            pltpu.VMEM((w_slots, width, head_dim), bf16),
            pltpu.VMEM(team_shape, bf16),
            pltpu.VMEM(team_shape, bf16),
            pltpu.VMEM((num_rows, width), bf16),
            pltpu.VMEM((num_rows * heads, half), f32),
            pltpu.VMEM((num_rows * heads, half), f32),
            pltpu.VMEM((num_rows * heads, half), f32),
            pltpu.VMEM((num_rows * heads, half), f32),
            pltpu.VMEM((num_rows, head_dim), f32),
            pltpu.VMEM((num_rows, head_dim), f32),
            pltpu.VMEM((num_rows, half), f32),
            pltpu.SemaphoreType.DMA((w_slots,)),
            pltpu.SemaphoreType.DMA((slots, TEAM)),
            pltpu.SemaphoreType.DMA((slots, TEAM)),
        ],
        compiler_params=pltpu.CompilerParams(vmem_limit_bytes=67043328),
        cost_estimate=pl.CostEstimate(flops=4 * num_rows * width * width, bytes_accessed=4 * width * width,
                                      transcendentals=0),
        name='attention_block',
    )(order, cache_len, hidden_in, norm_attn, norm_mlp, cos_t, sin_t, w_k, w_v, w_q, w_o,
      k_cache, v_cache)


def solution(mesh):
    row_spec = P(('dp', 'tp'), None)
    cache_spec = P(('dp', 'tp'), None, None)
    full_vec = P(None)
    full_mat = P(None, None)

    def per_device(hidden_in, k_cache, v_cache, cache_len, norm_attn, norm_mlp, w_q, w_k, w_v, w_o, w_gate, w_up, w_down):
        xn_mid, x_mid, k_new, v_new = attention_block(
            hidden_in, k_cache, v_cache, cache_len, norm_attn, norm_mlp, w_q, w_k, w_v, w_o)
        hidden_out = exchange_mlp(mesh.shape['tp'], xn_mid, x_mid, w_gate, w_up, w_down)
        return hidden_out, k_new, v_new

    return jax.shard_map(
        per_device,
        mesh=mesh,
        in_specs=(row_spec, cache_spec, cache_spec, P(('dp', 'tp')), full_vec, full_vec,
                  full_mat, full_mat, full_mat, full_mat, P(None, 'tp'), P(None, 'tp'), P('tp', None)),
        out_specs=(row_spec, row_spec, row_spec),
        check_vma=False,
    )
```

```python
import functools

import jax
import jax.numpy as jnp
from jax import lax
from jax.experimental import pallas as pl
from jax.experimental.pallas import tpu as pltpu
import numpy as np
from jax.sharding import PartitionSpec as P

ROWS = 128
PIECE = 64
SUB = 32


def mlp_kernel(num_tp, xn_ref, xmid_hbm, wg_hbm, wu_hbm, wd_hbm, out_ref,
               xg, hid, wg_buf, wu_buf, wd_buf, part, mate_out, mate_in, relay, from_x, from_y, x_mid,
               wg_sem, wu_sem, wd_sem, send_sem, recv_sem, x_sem):
    me = lax.axis_index('tp')
    mate = me + 1 - 2 * lax.rem(me, 2)
    xpeer = me + 2 - 4 * lax.rem(me // 2, 2)
    ypeer = me + 4 - 8 * (me // 4)

    h_tile = wg_buf.shape[2]
    n_tile = wd_buf.shape[2]
    h_steps = hid.shape[2] // h_tile
    n_steps = wd_hbm.shape[1] // n_tile
    groups = num_tp // 2
    gu_slots = wg_buf.shape[0]
    d_slots = wd_buf.shape[0]

    def gate_copy(step):
        cols = pl.ds(pl.multiple_of(lax.rem(step, h_steps) * h_tile, h_tile), h_tile)
        slot = lax.rem(step, gu_slots)
        return (pltpu.make_async_copy(wg_hbm.at[:, cols], wg_buf.at[slot], wg_sem.at[slot]),
                pltpu.make_async_copy(wu_hbm.at[:, cols], wu_buf.at[slot], wu_sem.at[slot]))

    def down_copy(step):
        cols = pl.ds(pl.multiple_of(lax.rem(step, n_steps) * n_tile, n_tile), n_tile)
        slot = lax.rem(step, d_slots)
        return pltpu.make_async_copy(wd_hbm.at[:, cols], wd_buf.at[slot], wd_sem.at[slot])

    for step in range(gu_slots):
        for copy in gate_copy(jnp.int32(step)):
            copy.start()
    for step in range(d_slots):
        down_copy(jnp.int32(step)).start()

    barrier = pltpu.get_barrier_semaphore()
    for peer in (mate, xpeer, ypeer):
        pl.semaphore_signal(barrier, inc=1, device_id={'tp': peer}, device_id_type=pl.DeviceIdType.MESH)
    pl.semaphore_wait(barrier, 3)

    count = [0]

    def remote(src, dst, peer):
        k = count[0]
        count[0] += 1
        return pltpu.make_async_remote_copy(
            src_ref=src, dst_ref=dst, send_sem=send_sem.at[k], recv_sem=recv_sem.at[k],
            device_id={'tp': peer}, device_id_type=pl.DeviceIdType.MESH)

    def rows_of(start, size):
        return xg.at[pl.ds(start, size), :]

    top, bot = xn_ref.at[pl.ds(0, PIECE), :], xn_ref.at[pl.ds(PIECE, PIECE), :]
    chunks = range(PIECE // SUB)

    def span(lead, c):
        return pl.ds(lead + c * SUB, SUB)

    own_mate = remote(xn_ref, rows_of(128, 128), mate)
    near_x = remote(top, rows_of(256, 64), xpeer)
    near_y = remote(bot, rows_of(320, 64), ypeer)
    diag_y = remote(rows_of(256, 64), rows_of(512, 64), ypeer)
    diag_x = remote(rows_of(320, 64), rows_of(576, 64), xpeer)
    far_x = [remote(xn_ref.at[span(PIECE, c), :], xg.at[span(768, c), :], xpeer) for c in chunks]
    far_y = [remote(xn_ref.at[span(0, c), :], xg.at[span(832, c), :], ypeer) for c in chunks]
    near_mate = remote(rows_of(256, 128), rows_of(384, 128), mate)
    diag_mate = remote(rows_of(512, 128), rows_of(640, 128), mate)
    far_mate = remote(rows_of(768, 128), rows_of(896, 128), mate)
    width = xn_ref.shape[1]
    quarters = 4
    side = [pl.ds(i * (width // quarters), width // quarters) for i in range(quarters)]
    pair = [[remote(mate_out.at[(g + 1) % 2, :, cols], mate_in.at[g, :, cols], mate) for cols in side]
            for g in range(groups)]
    high, low = pl.ds(0, PIECE), pl.ds(PIECE, PIECE)
    near_sx = [remote(part.at[1, high, cols], from_x.at[high, cols], xpeer) for cols in side]
    near_sy = [remote(part.at[1, low, cols], from_y.at[low, cols], ypeer) for cols in side]
    diag_sx = [remote(part.at[2, span(0, c), :], relay.at[span(PIECE, c), :], xpeer) for c in chunks]
    diag_sy = [remote(part.at[2, span(PIECE, c), :], relay.at[span(0, c), :], ypeer) for c in chunks]
    far_sx = [remote(part.at[3, span(0, c), :], from_x.at[span(PIECE, c), :], xpeer) for c in chunks]
    far_sy = [remote(part.at[3, span(PIECE, c), :], from_y.at[span(0, c), :], ypeer) for c in chunks]

    near_x.start()
    near_y.start()
    far_x[0].start()
    far_y[0].start()
    own_mate.start()
    mid_copy = pltpu.make_async_copy(xmid_hbm, x_mid, x_sem)
    mid_copy.start()
    xg[pl.ds(0, ROWS), :] = xn_ref[...]
    own_mate.wait_recv()

    def add_pair(g):
        for copy in pair[g]:
            copy.wait_recv()

        @pl.loop(0, ROWS // 8)
        def _(r):
            rows = pl.ds(pl.multiple_of(r * 8, 8), 8)
            part[g, rows, :] += mate_in[g, rows, :]

    def gather_near():
        near_x.wait_recv()
        diag_y.start()
        near_y.wait_recv()
        diag_x.start()
        far_x[1].start()
        far_y[1].start()
        near_mate.start()

    def gather_diag():
        diag_y.wait_recv()
        diag_x.wait_recv()
        diag_mate.start()

    def gather_far():
        for c in chunks:
            far_x[c].wait_recv()
            far_y[c].wait_recv()
        far_mate.start()

    def send_near(i):
        pair[1][i].wait_recv()

        @pl.loop(0, ROWS // 8)
        def _(r):
            rows = pl.ds(pl.multiple_of(r * 8, 8), 8)
            part[1, rows, side[i]] += mate_in[1, rows, side[i]]
        near_sx[i].start()
        near_sy[i].start()

    def send_near_and_gather():
        send_near(1)
        gather_diag()

    def send_diag():
        add_pair(2)
        for c in chunks:
            diag_sx[c].start()
            diag_sy[c].start()

    def free_slot(g):
        for copy in pair[g]:
            copy.wait_send()

    def start_diag():
        send_near(2)
        send_near(3)
        diag_mate.wait_recv()

    def start_far():
        send_diag()
        far_mate.wait_recv()

    def pass_on(c):
        diag_sy[c].wait_recv()
        part[3, span(0, c), :] += relay[span(0, c), :]
        far_sx[c].start()
        diag_sx[c].wait_recv()
        part[3, span(PIECE, c), :] += relay[span(PIECE, c), :]
        far_sy[c].start()

    before_h = {
        (0, h_steps - 1): gather_near,
        (1, 0): near_mate.wait_recv,
        (2, 0): start_diag,
        (2, h_steps - 1): gather_far,
        (3, 0): start_far,
    }
    before_n = {
        (1, n_steps - 4): lambda: send_near(0),
        (1, n_steps - 2): send_near_and_gather,
        (3, 0): lambda: free_slot(1),
        (0, 0): lambda: free_slot(2),
        (0, n_steps // 2): lambda: add_pair(3),
        (0, n_steps - 2): lambda: pass_on(0),
    }

    def run_hooks(table, g, step):
        for (hg, hs), action in table.items():
            @pl.when(jnp.logical_and(g == hg, step == hs))
            def _():
                action()

    @pl.loop(0, groups + 1)
    def _(turn):
        @pl.when(turn < groups)
        def _():
            rows = pl.ds(pl.multiple_of(turn * (2 * ROWS), 2 * ROWS), 2 * ROWS)
            keep = jnp.minimum(turn, 1)

            @pl.loop(0, h_steps)
            def _(j):
                run_hooks(before_h, turn, j)
                step = turn * h_steps + j
                slot = lax.rem(step, gu_slots)
                for copy in gate_copy(step):
                    copy.wait()
                gate_act = jnp.dot(xg[rows, :], wg_buf[slot], preferred_element_type=jnp.float32)
                up_act = jnp.dot(xg[rows, :], wu_buf[slot], preferred_element_type=jnp.float32)
                cols = pl.ds(pl.multiple_of(j * h_tile, h_tile), h_tile)
                hid[keep, :, cols] = (jax.nn.gelu(gate_act, approximate=True) * up_act).astype(jnp.bfloat16)

                @pl.when(step + gu_slots < groups * h_steps)
                def _():
                    for copy in gate_copy(step + gu_slots):
                        copy.start()

        @pl.when(turn > 0)
        def _():
            g = lax.rem(turn, groups)
            keep = jnp.minimum(g, 1)

            @pl.loop(0, n_steps)
            def _(n):
                run_hooks(before_n, g, n)
                step = (turn - 1) * n_steps + n
                slot = lax.rem(step, d_slots)
                down_copy(step).wait()
                res = jnp.dot(hid[keep], wd_buf[slot], preferred_element_type=jnp.float32)
                cols = pl.ds(pl.multiple_of(n * n_tile, n_tile), n_tile)
                part[g, :, cols] = res[:ROWS]
                mate_out[lax.rem(g + 1, 2), :, cols] = res[ROWS:]

                for hg in range(groups):
                    for i in range(quarters):
                        @pl.when(jnp.logical_and(g == hg, n == (i + 1) * n_steps // quarters - 1))
                        def _():
                            pair[hg][i].start()

                @pl.when(step + d_slots < groups * n_steps)
                def _():
                    down_copy(step + d_slots).start()


    add_pair(0)
    for copy in near_sx + near_sy:
        copy.wait_recv()
    mid_copy.wait()
    part[0] = part[0] + x_mid[...]
    part[0, pl.ds(0, PIECE), :] += from_x[pl.ds(0, PIECE), :]
    part[0, pl.ds(PIECE, PIECE), :] += from_y[pl.ds(PIECE, PIECE), :]
    for c in chunks[1:]:
        pass_on(c)
    for c in chunks:
        low, high = span(0, c), span(PIECE, c)
        far_sx[c].wait_recv()
        out_ref[high, :] = (part[0, high, :] + from_x[high, :]).astype(out_ref.dtype)
        far_sy[c].wait_recv()
        out_ref[low, :] = (part[0, low, :] + from_y[low, :]).astype(out_ref.dtype)
    for copy in ([own_mate, near_x, near_y, diag_y, diag_x, near_mate, diag_mate, far_mate]
                 + far_x + far_y + pair[3] + pair[0]
                 + near_sx + near_sy + diag_sx + diag_sy + far_sx + far_sy):
        copy.wait_send()


def exchange_mlp(num_tp, xn_mid, x_mid, w_gate, w_up, w_down):
    width = xn_mid.shape[1]
    hidden = w_gate.shape[1]
    h_tile, n_tile = 256, 512
    gu_slots, d_slots = 3, 3
    groups = num_tp // 2
    copies = 8 + 4 * groups + 8 + 6 * (PIECE // SUB)
    f32, bf16 = jnp.float32, jnp.bfloat16
    vmem = pl.BlockSpec(memory_space=pltpu.VMEM)
    hbm = pl.BlockSpec(memory_space=pl.ANY)
    return pl.pallas_call(
        functools.partial(mlp_kernel, num_tp),
        out_shape=jax.ShapeDtypeStruct((ROWS, width), bf16),
        in_specs=[vmem, hbm, hbm, hbm, hbm],
        out_specs=vmem,
        scratch_shapes=[
            pltpu.VMEM((num_tp * ROWS, width), bf16),
            pltpu.VMEM((2, 2 * ROWS, hidden), bf16),
            pltpu.VMEM((gu_slots, width, h_tile), bf16),
            pltpu.VMEM((gu_slots, width, h_tile), bf16),
            pltpu.VMEM((d_slots, hidden, n_tile), bf16),
            pltpu.VMEM((groups, ROWS, width), f32),
            pltpu.VMEM((2, ROWS, width), f32),
            pltpu.VMEM((groups, ROWS, width), f32),
            pltpu.VMEM((ROWS, width), f32),
            pltpu.VMEM((ROWS, width), f32),
            pltpu.VMEM((ROWS, width), f32),
            pltpu.VMEM((ROWS, width), f32),
            pltpu.SemaphoreType.DMA((gu_slots,)),
            pltpu.SemaphoreType.DMA((gu_slots,)),
            pltpu.SemaphoreType.DMA((d_slots,)),
            pltpu.SemaphoreType.DMA((copies,)),
            pltpu.SemaphoreType.DMA((copies,)),
            pltpu.SemaphoreType.DMA,
        ],
        compiler_params=pltpu.CompilerParams(
            collective_id=0, has_side_effects=True, vmem_limit_bytes=67043328),
        cost_estimate=pl.CostEstimate(flops=6 * num_tp * ROWS * width * hidden,
                                      bytes_accessed=6 * width * hidden * groups, transcendentals=0),
        name='exchange_mlp',
    )(xn_mid, x_mid, w_gate, w_up, w_down)


TEAM = 8
BLOCK = 128
AHEAD = 2
WIDE = 2


def attention_kernel(lens, row_ref, freq_ref, hid_ref, ga_ref, gm_ref, wk_hbm, wv_hbm, wq_hbm, wo_hbm,
                     kc_hbm, vc_hbm, xn_out, xmid_hbm, knew_out, vnew_out,
                     w_buf, k_buf, v_buf, xn, q_lo, q_hi, o_lo, o_hi, k_row, v_row, squares, cos_ref, sin_ref,
                     x_mid, rank_row, order_smem, w_sem, k_sem, v_sem, x_sem, order_sem):
    num_rows, width = hid_ref.shape
    head_dim = wk_hbm.shape[1]
    half = head_dim // 2
    heads = wq_hbm.shape[1] // head_dim
    tile_cols = WIDE * head_dim
    steps = heads // WIDE
    tiles = wo_hbm.shape[1] // tile_cols
    teams = num_rows // TEAM
    slots = k_buf.shape[0]
    w_slots = w_buf.shape[0]
    max_units = kc_hbm.shape[1] // BLOCK
    f32, bf16 = jnp.float32, jnp.bfloat16

    def tile_copy(src, tile, slot):
        cols = pl.ds(pl.multiple_of(tile * tile_cols, tile_cols), tile_cols)
        return pltpu.make_async_copy(src.at[:, cols], w_buf.at[slot], w_sem.at[slot])

    def head_copy(step):
        return tile_copy(wq_hbm, step, lax.rem(step + 1, w_slots))

    def out_copy(tile):
        return tile_copy(wo_hbm, tile, tile)

    first = [pltpu.make_async_copy(wk_hbm, w_buf.at[0, :, pl.ds(0, head_dim)], w_sem.at[0]),
             pltpu.make_async_copy(wv_hbm, w_buf.at[0, :, pl.ds(head_dim, head_dim)], w_sem.at[w_slots])]
    for copy in first:
        copy.start()
    head_copy(jnp.int32(0)).start()

    across = jnp.broadcast_to(row_ref[...].astype(f32), (num_rows, num_rows))
    down = jnp.transpose(across)
    row_id = lax.broadcasted_iota(jnp.int32, (num_rows, num_rows), 0)
    col_id = lax.broadcasted_iota(jnp.int32, (num_rows, num_rows), 1)
    is_ahead = (across < down) | ((across == down) & (col_id < row_id))
    rank = jnp.sum(jnp.where(is_ahead, 1.0, 0.0), axis=1, keepdims=True)
    placed = jnp.where(rank == col_id.astype(f32), row_id.astype(f32), 0.0)
    rank_row[...] = jnp.sum(placed, axis=0, keepdims=True).astype(jnp.int32)
    order_copy = pltpu.make_async_copy(rank_row, order_smem, order_sem)
    order_copy.start()
    angles = down * freq_ref[...]
    cos_ref[...] = jnp.cos(angles)
    sin_ref[...] = jnp.sin(angles)
    order_copy.wait()

    def units_of(team):
        longest = lens[order_smem[0, team * TEAM + TEAM - 1]]
        return jnp.maximum((longest + BLOCK - 1) // BLOCK, 1)

    def key_copy(team, r, n):
        slot, span = lax.rem(team, slots), pl.ds(0, n * BLOCK)
        return pltpu.make_async_copy(kc_hbm.at[order_smem[0, team * TEAM + r], span, :],
                                     k_buf.at[slot, r, span, :], k_sem.at[slot, r])

    def value_copy(team, r, n):
        slot, span = lax.rem(team, slots), pl.ds(0, n * BLOCK)
        return pltpu.make_async_copy(vc_hbm.at[order_smem[0, team * TEAM + r], span, :],
                                     v_buf.at[slot, r, span, :], v_sem.at[slot, r])

    def fetch(team):
        units = units_of(team)
        for n in range(1, max_units + 1):
            @pl.when(units == n)
            def _():
                for r in range(TEAM):
                    key_copy(team, r, n).start()
                    value_copy(team, r, n).start()

    def normalise(src, gain_ref, dst):
        gain = 1.0 + gain_ref[...].astype(f32)[None, :]

        @pl.loop(0, num_rows // 16)
        def _(i):
            rows = pl.ds(pl.multiple_of(i * 16, 16), 16)
            wide = src[rows, :].astype(f32)
            inv = lax.rsqrt(jnp.mean(wide * wide, axis=-1, keepdims=True) + 1e-6)
            dst[rows, :] = (wide * inv * gain).astype(bf16)

    normalise(hid_ref, ga_ref, xn)

    def rotate(lin):
        low, high = lin[:, :half], lin[:, half:]
        cos_t, sin_t = cos_ref[...], sin_ref[...]
        return low * cos_t - high * sin_t, high * cos_t + low * sin_t

    for copy in first:
        copy.wait()
    head_copy(jnp.int32(1)).start()
    both = jnp.dot(xn[...], w_buf[0], preferred_element_type=f32)
    low, high = rotate(both[:, :head_dim])
    key = jnp.concatenate([low, high], axis=-1).astype(bf16)
    knew_out[...] = key
    k_row[...] = key.astype(f32)
    value = both[:, head_dim:].astype(bf16)
    vnew_out[...] = value
    v_row[...] = value.astype(f32)

    @pl.loop(0, steps)
    def _(step):
        head_copy(step).wait()

        @pl.when(step + AHEAD < steps)
        def _():
            head_copy(step + AHEAD).start()
        for team in range(slots - 1):
            @pl.when(step == steps - AHEAD + team)
            def _():
                fetch(jnp.int32(team))
        lin = jnp.dot(xn[...], w_buf[lax.rem(step + 1, w_slots)], preferred_element_type=f32)
        for i in range(WIDE):
            low, high = rotate(lin[:, i * head_dim:(i + 1) * head_dim])
            spots = pl.ds(step * WIDE + i, num_rows, stride=heads)
            q_lo[spots, :] = (low * head_dim ** -0.5).astype(bf16).astype(f32)
            q_hi[spots, :] = (high * head_dim ** -0.5).astype(bf16).astype(f32)

    def attend(team, n):
        slot = lax.rem(team, slots)
        size = n * BLOCK
        rows = [order_smem[0, team * TEAM + r] for r in range(TEAM)]
        spans = [pl.ds(pl.multiple_of(row * heads, heads), heads) for row in rows]
        for r in range(TEAM):
            key_copy(team, r, n).wait()
        wide = [jnp.concatenate([q_lo[span, :], q_hi[span, :]], axis=-1) for span in spans]
        scores = [lax.dot_general(wide[r].astype(bf16), k_buf[slot, r, pl.ds(0, size), :], (((1,), (1,)), ((), ())),
                                  preferred_element_type=f32) for r in range(TEAM)]
        for r in range(TEAM):
            value_copy(team, r, n).wait()
        place = lax.broadcasted_iota(jnp.int32, scores[0].shape, 1)
        probs, news = [], []
        for r in range(TEAM):
            score = jnp.where(place < lens[rows[r]], scores[r], -jnp.inf)
            fresh = jnp.sum(wide[r] * k_row[pl.ds(rows[r], 1), :], axis=-1, keepdims=True)
            peak = jnp.maximum(jnp.max(score, axis=-1, keepdims=True), fresh)
            weight = jnp.exp(score - peak)
            fresh = jnp.exp(fresh - peak)
            scale = 1.0 / (jnp.sum(weight, axis=-1, keepdims=True) + fresh)
            probs.append((weight * scale).astype(bf16))
            news.append((fresh * scale).astype(bf16).astype(f32))
        for r in range(TEAM):
            mixed = jnp.dot(probs[r], v_buf[slot, r, pl.ds(0, size), :], preferred_element_type=f32)
            mixed = mixed + news[r] * v_row[pl.ds(rows[r], 1), :]
            mixed = mixed.astype(bf16).astype(f32)
            o_lo[spans[r], :] = mixed[:, :half]
            o_hi[spans[r], :] = mixed[:, half:]

    share = teams // tiles

    @pl.loop(0, teams)
    def _(team):
        @pl.when(team + slots - 1 < teams)
        def _():
            fetch(team + slots - 1)
        @pl.when(lax.rem(team, share) == 0)
        def _():
            out_copy(team // share).start()
        units = units_of(team)
        for n in range(1, max_units + 1):
            @pl.when(units == n)
            def _():
                attend(team, n)

    for head in range(heads):
        spots = pl.ds(head, num_rows, stride=heads)
        xn[:, pl.ds(head * head_dim, half)] = o_lo[spots, :].astype(bf16)
        xn[:, pl.ds(head * head_dim + half, half)] = o_hi[spots, :].astype(bf16)
    squares[...] = jnp.zeros_like(squares)

    def mid_copy(tile):
        cols = pl.ds(pl.multiple_of(tile * tile_cols, tile_cols), tile_cols)
        return pltpu.make_async_copy(x_mid.at[:, cols], xmid_hbm.at[:, cols], x_sem.at[tile])

    @pl.loop(0, tiles)
    def _(tile):
        out_copy(tile).wait()
        cols = pl.ds(pl.multiple_of(tile * tile_cols, tile_cols), tile_cols)
        mixed = hid_ref[:, cols].astype(f32) + jnp.dot(xn[...], w_buf[tile], preferred_element_type=f32)
        x_mid[:, cols] = mixed
        mid_copy(tile).start()
        mixed = mixed * mixed
        squares[...] += sum(mixed[:, i * half:(i + 1) * half] for i in range(tile_cols // half))

    gain = 1.0 + gm_ref[...].astype(f32)[None, :]

    @pl.loop(0, num_rows // 16)
    def _(i):
        rows = pl.ds(pl.multiple_of(i * 16, 16), 16)
        inv = lax.rsqrt(jnp.sum(squares[rows, :], axis=-1, keepdims=True) * (1.0 / width) + 1e-6)
        xn_out[rows, :] = (x_mid[rows, :] * inv * gain).astype(bf16)

    for tile in range(tiles):
        mid_copy(jnp.int32(tile)).wait()


def attention_block(hidden_in, k_cache, v_cache, cache_len, norm_attn, norm_mlp, w_q, w_k, w_v, w_o):
    num_rows, width = hidden_in.shape
    head_dim = w_k.shape[1]
    half = head_dim // 2
    heads = w_q.shape[1] // head_dim
    inv_freq = (10000.0 ** (-2.0 * np.arange(half) / head_dim)).astype(np.float32)
    slots, tiles = 3, w_o.shape[1] // (WIDE * head_dim)
    f32, bf16 = jnp.float32, jnp.bfloat16
    vmem = pl.BlockSpec(memory_space=pltpu.VMEM)
    smem = pl.BlockSpec(memory_space=pltpu.SMEM)
    hbm = pl.BlockSpec(memory_space=pl.ANY)
    team_shape = (slots, TEAM, k_cache.shape[1], head_dim)
    return pl.pallas_call(
        attention_kernel,
        out_shape=[jax.ShapeDtypeStruct((num_rows, width), bf16), jax.ShapeDtypeStruct((num_rows, width), f32),
                   jax.ShapeDtypeStruct((num_rows, head_dim), bf16), jax.ShapeDtypeStruct((num_rows, head_dim), bf16)],
        in_specs=[smem, vmem, vmem, vmem, vmem, vmem, hbm, hbm, hbm, hbm, hbm, hbm],
        out_specs=[vmem, hbm, vmem, vmem],
        scratch_shapes=[
            pltpu.VMEM((tiles, width, WIDE * head_dim), bf16),
            pltpu.VMEM(team_shape, bf16),
            pltpu.VMEM(team_shape, bf16),
            pltpu.VMEM((num_rows, width), bf16),
            pltpu.VMEM((num_rows * heads, half), f32),
            pltpu.VMEM((num_rows * heads, half), f32),
            pltpu.VMEM((num_rows * heads, half), f32),
            pltpu.VMEM((num_rows * heads, half), f32),
            pltpu.VMEM((num_rows, head_dim), f32),
            pltpu.VMEM((num_rows, head_dim), f32),
            pltpu.VMEM((num_rows, half), f32),
            pltpu.VMEM((num_rows, half), f32),
            pltpu.VMEM((num_rows, half), f32),
            pltpu.VMEM((num_rows, width), f32),
            pltpu.VMEM((1, num_rows), jnp.int32),
            pltpu.SMEM((1, num_rows), jnp.int32),
            pltpu.SemaphoreType.DMA((tiles + 1,)),
            pltpu.SemaphoreType.DMA((slots, TEAM)),
            pltpu.SemaphoreType.DMA((slots, TEAM)),
            pltpu.SemaphoreType.DMA((tiles,)),
            pltpu.SemaphoreType.DMA,
        ],
        compiler_params=pltpu.CompilerParams(vmem_limit_bytes=67043328),
        cost_estimate=pl.CostEstimate(flops=4 * num_rows * width * width, bytes_accessed=4 * width * width,
                                      transcendentals=0),
        name='attention_block',
    )(cache_len, cache_len[None, :], inv_freq[None, :], hidden_in, norm_attn, norm_mlp, w_k, w_v, w_q, w_o,
      k_cache, v_cache)


def solution(mesh):
    row_spec = P(('dp', 'tp'), None)
    cache_spec = P(('dp', 'tp'), None, None)
    full_vec = P(None)
    full_mat = P(None, None)

    def per_device(hidden_in, k_cache, v_cache, cache_len, norm_attn, norm_mlp, w_q, w_k, w_v, w_o, w_gate, w_up, w_down):
        xn_mid, x_mid, k_new, v_new = attention_block(
            hidden_in, k_cache, v_cache, cache_len, norm_attn, norm_mlp, w_q, w_k, w_v, w_o)
        hidden_out = exchange_mlp(mesh.shape['tp'], xn_mid, x_mid, w_gate, w_up, w_down)
        return hidden_out, k_new, v_new

    return jax.shard_map(
        per_device,
        mesh=mesh,
        in_specs=(row_spec, cache_spec, cache_spec, P(('dp', 'tp')), full_vec, full_vec,
                  full_mat, full_mat, full_mat, full_mat, P(None, 'tp'), P(None, 'tp'), P('tp', None)),
        out_specs=(row_spec, row_spec, row_spec),
        check_vma=False,
    )
```
